32 devices in a mesh: zero: 4 (over z), width: 4 (over y, x), unit: 2 (over core).
Axes of the slice: x: 2, y: 2, z: 4, core: 2. Of those that a mesh axis runs over, the one named last changes fastest.
Arguments:
- train_query: bfloat16 [8192, 4096], P(('unit', 'zero'), 'width'), parts along dimension 0, may hold values from -0.125 to 0.125
- low_query: bfloat16 [8192, 16], P(('unit', 'zero')), parts along dimension 0, may hold values from -0.09375 to 0.09375
- high_query: bfloat16 [32, 4096], P('unit', 'width'), parts along dimension 0, may hold values from -1.5 to 1.5
- train_key: bfloat16 [8192, 4096], P(('unit', 'zero'), 'width'), parts along dimension 0, may hold values from -0.125 to 0.125
- low_key: bfloat16 [8192, 16], P(('unit', 'zero')), parts along dimension 0, may hold values from -0.09375 to 0.09375
- high_key: bfloat16 [32, 4096], P('unit', 'width'), parts along dimension 0, may hold values from -1.5 to 1.5
- train_value: bfloat16 [8192, 4096], P(('unit', 'zero'), 'width'), parts along dimension 0, may hold values from -0.125 to 0.125
- low_value: bfloat16 [8192, 16], P(('unit', 'zero')), parts along dimension 0, may hold values from -0.09375 to 0.09375
- high_value: bfloat16 [32, 4096], P('unit', 'width'), parts along dimension 0, may hold values from -1.5 to 1.5
- norm_train: float32 [8192], P(('unit', 'zero', 'width')), parts along dimension 0, may hold values from 0.25 to 1.75
- norm_step: float32 [8192], P(('unit', 'zero', 'width')), parts along dimension 0, may hold values from -0.3 to 0.3
Outputs:
- serve_query: bfloat16 [8192, 4096], P('unit', 'width'), parts along dimension 0
- serve_key: bfloat16 [8192, 4096], P('unit', 'width'), parts along dimension 0
- serve_value: bfloat16 [8192, 4096], P('unit', 'width'), parts along dimension 0
- factor_query: float32 [8192], P(('unit', 'width')), parts along dimension 0
- factor_key: float32 [8192], P(('unit', 'width')), parts along dimension 0
- factor_value: float32 [8192], P(('unit', 'width')), parts along dimension 0
- serve_norm: bfloat16 [8192], P('unit'), parts along dimension 0
The draws below stay inside these ranges and needn't reach their ends.
There are 2 independent parts, one for each index of `unit`. The reference program is written for one: setup_inputs(seed, part) draws one part's arguments, and reference() takes and returns one part's arrays. A program takes and returns all parts, laid end to end along the dimension named above; each array names one. Nothing has to cross between parts.
All inputs are finite; a program needn't handle non-finite values. Where the reference program divides by a largest or mean magnitude, that divisor is 1e-20 or more.
Results may differ from the reference program's by a relative error of at most 0.001.
Values may be sent and summed in bfloat16 or wider, within the bound.
No kernel may reach another device: no remote copies, remote signals or barrier semaphores. Data moves between devices by JAX's collectives and lax.ppermute only.
A program may use at most 128 MiB of HBM per device.

```python
import jax
import jax.numpy as jnp

D_MODEL = 4096
Q_DIM = 4096
KV_DIM = 4096
RANK = 16


def with_spikes(drawn, key, source, target, parts, factor):
    owner, partner = [(jnp.arange(drawn.shape[axis_at]) // (drawn.shape[axis_at] // parts)).reshape([-1 if axis == axis_at else 1 for axis in range(drawn.ndim)]) for axis_at in (source, target)]
    chosen = jax.random.permutation(key, parts)[partner]
    strong = (owner == chosen) | (owner == (partner + parts // 2) % parts)
    return jnp.where(strong, factor * drawn, drawn)


def level_of(rng, dims, split, least, largest):
    factor_of = 1.0
    for axis_at, blocks in split:
        steps = jax.random.uniform(jax.random.fold_in(jax.random.fold_in(rng, 6), axis_at), (blocks,), jnp.float32, least / len(split), largest / len(split))
        factor_of = factor_of * jnp.repeat(jnp.exp(steps), dims[axis_at] // blocks).reshape((-1,) + (1,) * (len(dims) - 1 - axis_at))
    return factor_of


def scatter_about(key, dims, deviation, most, split=(), kind=jnp.bfloat16):
    entries = deviation * jax.random.normal(key, dims, jnp.float32)
    if split:
        entries = entries * level_of(key, dims, split, -0.22, 0.18)
    return jnp.clip(entries, -most, most).astype(kind)


def noise_with(rng, shape, scale, most, split, heavy, held_as=jnp.bfloat16):
    array = scale * jax.random.normal(rng, shape, jnp.float32)
    if split:
        array = array * level_of(rng, shape, split, -0.22, 0.18)
    return jnp.clip(with_spikes(array, jax.random.fold_in(rng, 3), *heavy), -most, most).astype(held_as)


def setup_inputs(seed: int = 0, part: int = 0) -> dict:
    seeds = jax.random.split(jax.random.key(seed), 12)
    part_splits = jax.random.split(jax.random.fold_in(seeds[11], part), 12)
    train_query = noise_with(part_splits[0], (D_MODEL, Q_DIM), D_MODEL ** -0.5, 0.125, ((0, 4), (1, 4)), (0, 1, 4, 2.0))
    low_query = scatter_about(part_splits[1], (D_MODEL, RANK), D_MODEL ** -0.5, 0.09375, ((0, 4),))
    high_query = scatter_about(part_splits[2], (RANK, Q_DIM), RANK ** -0.5, 1.5, ((1, 4),))
    train_key = noise_with(part_splits[3], (D_MODEL, KV_DIM), D_MODEL ** -0.5, 0.125, ((0, 4), (1, 4)), (0, 1, 4, 2.0))
    low_key = scatter_about(part_splits[4], (D_MODEL, RANK), D_MODEL ** -0.5, 0.09375, ((0, 4),))
    high_key = scatter_about(part_splits[5], (RANK, KV_DIM), RANK ** -0.5, 1.5, ((1, 4),))
    train_value = noise_with(part_splits[6], (D_MODEL, KV_DIM), D_MODEL ** -0.5, 0.125, ((0, 4), (1, 4)), (0, 1, 4, 2.0))
    low_value = scatter_about(part_splits[7], (D_MODEL, RANK), D_MODEL ** -0.5, 0.09375, ((0, 4),))
    high_value = scatter_about(part_splits[8], (RANK, KV_DIM), RANK ** -0.5, 1.5, ((1, 4),))
    norm_train = jnp.clip(1.0 + 0.15 * jax.random.normal(part_splits[9], (D_MODEL,), jnp.float32), 0.25, 1.75)
    norm_step = jnp.clip(jax.random.uniform(part_splits[10], (D_MODEL,), jnp.float32, -0.3, 0.3) * level_of(part_splits[10], (D_MODEL,), ((0, 16),), -0.4, 0.0), -0.3, 0.3)
    return dict(train_query=train_query, low_query=low_query, high_query=high_query, train_key=train_key, low_key=low_key, high_key=high_key, train_value=train_value, low_value=low_value, high_value=high_value, norm_train=norm_train, norm_step=norm_step)


mix_rate = 1.0


def reference(train_query, low_query, high_query, train_key, low_key, high_key, train_value, low_value, high_value, norm_train, norm_step):
    fresh_query = train_query.astype(jnp.float32) + mix_rate * jnp.dot(low_query, high_query, preferred_element_type=jnp.float32)
    fresh_key = train_key.astype(jnp.float32) + mix_rate * jnp.dot(low_key, high_key, preferred_element_type=jnp.float32)
    fresh_value = train_value.astype(jnp.float32) + mix_rate * jnp.dot(low_value, high_value, preferred_element_type=jnp.float32)
    factor_query = jnp.max(jnp.abs(fresh_query), axis=0)
    serve_query = (fresh_query / factor_query).astype(jnp.bfloat16)
    factor_key = jnp.max(jnp.abs(fresh_key), axis=0)
    serve_key = (fresh_key / factor_key).astype(jnp.bfloat16)
    factor_value = jnp.max(jnp.abs(fresh_value), axis=0)
    serve_value = (fresh_value / factor_value).astype(jnp.bfloat16)
    serve_norm = (norm_train + norm_step).astype(jnp.bfloat16)
    return serve_query, serve_key, serve_value, factor_query, factor_key, factor_value, serve_norm
```

```python
import functools

import jax
import jax.numpy as jnp
from jax import lax
from jax.experimental import pallas as pl
from jax.experimental.pallas import tpu as pltpu
from jax.sharding import PartitionSpec as P

mix_rate = 1.0


HBM = pltpu.MemorySpace.HBM
VMEM = pltpu.MemorySpace.VMEM


def tile_of(rows, most=256):
    tile = min(rows, most)
    while rows % tile:
        tile //= 2
    return tile


def merged(train, low_t, high):
    step = lax.dot_general(
        low_t, high, (((0,), (0,)), ((), ())), preferred_element_type=jnp.float32
    )
    return train.astype(jnp.float32) + mix_rate * step


def top_kernel(tq, tk, tv, lq, lk, lv, hq, hk, hv, norm, out, acc):
    step = pl.program_id(0)
    for index, (t, l, h) in enumerate(((tq, lq, hq), (tk, lk, hk), (tv, lv, hv))):
        size = jnp.abs(merged(t[...], l[...], h[...]))
        rows, cols = size.shape
        best = jnp.max(size.reshape(rows // 8, 8, cols), axis=0)

        @pl.when(step == 0)
        def _():
            acc[index] = best

        @pl.when(step > 0)
        def _():
            acc[index] = jnp.maximum(acc[index], best)

    @pl.when(step == pl.num_programs(0) - 1)
    def _():
        for index in range(3):
            out[pl.ds(index, 1), :] = jnp.max(acc[index], axis=0, keepdims=True)
        out[pl.ds(3, 1), :] = norm[...]


def column_tops(trains, lows, highs, norm):
    rows, cols = trains[0].shape
    rank = lows[0].shape[0]
    tile = tile_of(rows)
    return pl.pallas_call(
        top_kernel,
        grid=(rows // tile,),
        in_specs=[pl.BlockSpec((tile, cols), lambda i: (i, 0))] * 3
        + [pl.BlockSpec((rank, tile), lambda i: (0, i))] * 3
        + [pl.BlockSpec((rank, cols), lambda i: (0, 0))] * 3
        + [pl.BlockSpec((1, cols), lambda i: (0, 0))],
        out_specs=pl.BlockSpec((8, cols), lambda i: (0, 0)),
        out_shape=jax.ShapeDtypeStruct((8, cols), jnp.float32),
        scratch_shapes=[pltpu.VMEM((3, 8, cols), jnp.float32)],
        name="tops",
        cost_estimate=pl.CostEstimate(
            flops=3 * 2 * rows * cols * rank, bytes_accessed=6 * rows * cols, transcendentals=0
        ),
    )(*trains, *lows, *highs, norm)


def join_kernel(count, place, *refs):
    parts, (factor, norm) = refs[:count], refs[count:]
    total = parts[0][...]
    for part in parts[1:]:
        total = jnp.maximum(total, part[...])
    factor[...] = total
    for shift, part in enumerate(parts):
        owner = lax.rem(place[0] - shift + count, count)
        norm[pl.ds(owner, 1), :] = part[pl.ds(3, 1), :]


def join_tops(place, parts):
    count, cols = len(parts), parts[0].shape[1]
    return pl.pallas_call(
        functools.partial(join_kernel, count),
        in_specs=[pl.BlockSpec(memory_space=pltpu.MemorySpace.SMEM)]
        + [pl.BlockSpec(memory_space=VMEM)] * count,
        out_specs=[pl.BlockSpec(memory_space=VMEM)] * 2,
        out_shape=[
            jax.ShapeDtypeStruct((8, cols), jnp.float32),
            jax.ShapeDtypeStruct((max(8, count), cols), jnp.float32),
        ],
        name="join",
    )(place, *parts)


def scale_kernel(index, train, low_t, high, factor, serve):
    fresh = merged(train[...], low_t[...], high[...])
    serve[...] = (fresh / factor[pl.ds(index, 1), :]).astype(serve.dtype)


def scaled(index, train, low_t, high, factor, low_at=0):
    rows, cols = train.shape
    rank = high.shape[0]
    tile = tile_of(rows)
    first = low_at // tile
    return pl.pallas_call(
        functools.partial(scale_kernel, index),
        grid=(rows // tile,),
        in_specs=[
            pl.BlockSpec((tile, cols), lambda i: (i, 0)),
            pl.BlockSpec((rank, tile), lambda i: (0, i + first)),
            pl.BlockSpec((rank, cols), lambda i: (0, 0)),
            pl.BlockSpec((8, cols), lambda i: (0, 0)),
        ],
        out_specs=pl.BlockSpec((tile, cols), lambda i: (i, 0)),
        out_shape=jax.ShapeDtypeStruct((rows, cols), jnp.bfloat16),
        name="scale",
        cost_estimate=pl.CostEstimate(
            flops=2 * rows * cols * rank, bytes_accessed=4 * rows * cols, transcendentals=0
        ),
    )(train, low_t, high, factor)


def place_kernel(plan, count, place, *refs):
    sources, out, buffers = refs[1 : 1 + len(plan)], refs[1 + len(plan)], refs[2 + len(plan) :]
    slots, (read, written) = buffers[:-2], buffers[-2:]
    mine = place[0]
    for index, (shift, at, shard) in enumerate(plan):
        owner = mine + shift
        rows = sources[index].shape[0]
        pieces = slots[index].shape[0]
        part = rows // pieces

        @pl.when((owner >= 0) & (owner < count))
        def _(index=index, owner=owner, pieces=pieces, part=part, at=at, shard=shard):
            loads = [
                pltpu.make_async_copy(
                    sources[index].at[pl.ds(p * part, part)], slots[index].at[p], read.at[index, p]
                )
                for p in range(pieces)
            ]
            for load in loads:
                load.start()
            stores = []
            for p, load in enumerate(loads):
                start = pl.multiple_of(owner * shard + at + p * part, part)
                load.wait()
                store = pltpu.make_async_copy(
                    slots[index].at[p], out.at[pl.ds(start, part)], written.at[index, p]
                )
                store.start()
                stores.append(store)
            for store in stores:
                store.wait()


def placed(place, out, count, plan, sources):
    cols = out.shape[1]
    pieces = max(1, max(source.shape[0] // tile_of(source.shape[0]) for source in sources))
    return pl.pallas_call(
        functools.partial(place_kernel, plan, count),
        in_specs=[pl.BlockSpec(memory_space=pltpu.MemorySpace.SMEM)]
        + [pl.BlockSpec(memory_space=HBM)] * (1 + len(sources)),
        out_specs=pl.BlockSpec(memory_space=HBM),
        out_shape=jax.ShapeDtypeStruct(out.shape, out.dtype),
        scratch_shapes=[
            pltpu.VMEM(
                (
                    source.shape[0] // tile_of(source.shape[0]),
                    tile_of(source.shape[0]),
                    cols,
                ),
                source.dtype,
            )
            for source in sources
        ]
        + [pltpu.SemaphoreType.DMA((len(sources), pieces))] * 2,
        input_output_aliases={1: 0},
        name="place",
        cost_estimate=pl.CostEstimate(
            flops=sum(source.size for source in sources),
            bytes_accessed=sum(4 * source.size for source in sources),
            transcendentals=0,
        ),
    )(place, out, *sources)


def own_kernel(index, place, train, low_t, high, factor, serve, out):
    del place
    fresh = merged(train[...], low_t[...], high[...])
    block = (fresh / factor[pl.ds(index, 1), :]).astype(serve.dtype)
    serve[...] = block
    out[...] = block


def own_scaled(index, place, count, train, low_t, high, factor):
    rows, cols = train.shape
    rank = high.shape[0]
    tile = tile_of(rows)
    steps = rows // tile
    return pl.pallas_call(
        functools.partial(own_kernel, index),
        grid_spec=pltpu.PrefetchScalarGridSpec(
            num_scalar_prefetch=1,
            grid=(steps,),
            in_specs=[
                pl.BlockSpec((tile, cols), lambda i, place: (i, 0)),
                pl.BlockSpec((rank, tile), lambda i, place: (0, i)),
                pl.BlockSpec((rank, cols), lambda i, place: (0, 0)),
                pl.BlockSpec((8, cols), lambda i, place: (0, 0)),
            ],
            out_specs=[
                pl.BlockSpec((tile, cols), lambda i, place: (i, 0)),
                pl.BlockSpec((tile, cols), lambda i, place: (place[0] * steps + i, 0)),
            ],
        ),
        out_shape=[
            jax.ShapeDtypeStruct((rows, cols), jnp.bfloat16),
            jax.ShapeDtypeStruct((count * rows, cols), jnp.bfloat16),
        ],
        name="own",
        cost_estimate=pl.CostEstimate(
            flops=2 * rows * cols * rank, bytes_accessed=6 * rows * cols, transcendentals=0
        ),
    )(place, train, low_t, high, factor)


def per_device(
    count,
    train_query,
    low_query,
    high_query,
    train_key,
    low_key,
    high_key,
    train_value,
    low_value,
    high_value,
    norm_train,
    norm_step,
):
    rows, cols = train_query.shape
    half = rows // 2
    place = lax.axis_index("zero").astype(jnp.int32).reshape(1)
    lows = (low_query.T, low_key.T, low_value.T)
    highs = (high_query, high_key, high_value)
    trains = (train_query, train_key, train_value)

    def left(x, hop):
        return lax.ppermute(x, "zero", [(i, i - 1) for i in range(1, count - hop + 1)])

    def right(x, hop):
        return lax.ppermute(x, "zero", [(i, i + 1) for i in range(hop - 1, count - 1)])

    halves = (train_query[:half], train_query[half:])
    raw = [(left(halves[0], 1), right(halves[0], 1))]
    norm = jnp.pad(norm_train + norm_step, (0, cols - norm_train.shape[0])).reshape(1, cols)
    tops = column_tops(trains, lows, highs, norm)
    parts = [tops] + [
        lax.ppermute(tops, "zero", [(i, (i + s) % count) for i in range(count)])
        for s in range(1, count)
    ]
    raw.append((left(halves[1], 1), right(halves[1], 1)))
    near = (left(lows[0], 1), right(lows[0], 1))
    factor, norms = join_tops(place, parts)

    outs = [None] * 3
    sends = [None] * 3
    for index in (1, 2, 0):
        sends[index], outs[index] = own_scaled(
            index, place, count, trains[index], lows[index], highs[index], factor
        )
    pieces = [
        (
            0,
            p * half,
            tuple(
                scaled(0, got, low, high_query, factor, p * half) for got, low in zip(raw[p], near)
            ),
        )
        for p in range(2)
    ]
    for index in (1, 2):
        pieces.append((index, 0, (left(sends[index], 1), right(sends[index], 1))))

    for hop in range(1, count):
        later = []
        for index, at, (from_right, from_left) in pieces:
            if hop + 1 < count:
                later.append((index, at, (left(from_right, hop + 1), right(from_left, hop + 1))))
            outs[index] = placed(
                place,
                outs[index],
                count,
                ((hop, at, rows), (-hop, at, rows)),
                (from_right, from_left),
            )
        pieces = later

    size = norm_train.shape[0]
    wide = lax.all_gather(norms[:count, :size].astype(jnp.bfloat16), "width", axis=1, tiled=True)
    serve_norm = wide.reshape(-1)
    return (*outs, factor[0], factor[1], factor[2], serve_norm)


def solution(mesh):
    return jax.shard_map(
        functools.partial(per_device, mesh.shape["zero"]),
        mesh=mesh,
        in_specs=(
            P(("unit", "zero"), "width"),
            P(("unit", "zero"), None),
            P("unit", "width"),
            P(("unit", "zero"), "width"),
            P(("unit", "zero"), None),
            P("unit", "width"),
            P(("unit", "zero"), "width"),
            P(("unit", "zero"), None),
            P("unit", "width"),
            P(("unit", "zero", "width")),
            P(("unit", "zero", "width")),
        ),
        out_specs=(
            P("unit", "width"),
            P("unit", "width"),
            P("unit", "width"),
            P(("unit", "width")),
            P(("unit", "width")),
            P(("unit", "width")),
            P("unit"),
        ),
        check_vma=False,
    )
```

```python
import functools

import jax
import jax.numpy as jnp
from jax import lax
from jax.experimental import pallas as pl
from jax.experimental.pallas import tpu as pltpu
from jax.sharding import PartitionSpec as P

mix_rate = 1.0


HBM = pltpu.MemorySpace.HBM
VMEM = pltpu.MemorySpace.VMEM


def tile_of(rows, most=256):
    tile = min(rows, most)
    while rows % tile:
        tile //= 2
    return tile


def merged(train, low_t, high):
    step = lax.dot_general(
        low_t, high, (((0,), (0,)), ((), ())), preferred_element_type=jnp.float32
    )
    return train.astype(jnp.float32) + mix_rate * step


def top_kernel(tq, tk, tv, lq, lk, lv, hq, hk, hv, norm, out, acc):
    step = pl.program_id(0)
    for index, (t, l, h) in enumerate(((tq, lq, hq), (tk, lk, hk), (tv, lv, hv))):
        size = jnp.abs(merged(t[...], l[...], h[...]))
        rows, cols = size.shape
        best = jnp.max(size.reshape(rows // 8, 8, cols), axis=0)

        @pl.when(step == 0)
        def _():
            acc[index] = best

        @pl.when(step > 0)
        def _():
            acc[index] = jnp.maximum(acc[index], best)

    @pl.when(step == pl.num_programs(0) - 1)
    def _():
        for index in range(3):
            out[pl.ds(index, 1), :] = jnp.max(acc[index], axis=0, keepdims=True)
        out[pl.ds(3, 1), :] = norm[...]


def column_tops(trains, lows, highs, norm):
    rows, cols = trains[0].shape
    rank = lows[0].shape[0]
    tile = tile_of(rows)
    return pl.pallas_call(
        top_kernel,
        grid=(rows // tile,),
        in_specs=[pl.BlockSpec((tile, cols), lambda i: (i, 0))] * 3
        + [pl.BlockSpec((rank, tile), lambda i: (0, i))] * 3
        + [pl.BlockSpec((rank, cols), lambda i: (0, 0))] * 3
        + [pl.BlockSpec((1, cols), lambda i: (0, 0))],
        out_specs=pl.BlockSpec((4, cols), lambda i: (0, 0)),
        out_shape=jax.ShapeDtypeStruct((4, cols), jnp.float32),
        scratch_shapes=[pltpu.VMEM((3, 8, cols), jnp.float32)],
        compiler_params=pltpu.CompilerParams(vmem_limit_bytes=16 * 2**20),
        name="tops",
        cost_estimate=pl.CostEstimate(
            flops=3 * 2 * rows * cols * rank, bytes_accessed=6 * rows * cols, transcendentals=0
        ),
    )(*trains, *lows, *highs, norm)


def join_kernel(count, place, *refs):
    parts, (factor, norm) = refs[:count], refs[count:]
    total = parts[0][...]
    for part in parts[1:]:
        total = jnp.maximum(total, part[...])
    factor[...] = total
    for shift, part in enumerate(parts):
        owner = lax.rem(place[0] - shift + count, count)
        norm[pl.ds(owner, 1), :] = part[pl.ds(3, 1), :]


def join_tops(place, parts):
    count, cols = len(parts), parts[0].shape[1]
    return pl.pallas_call(
        functools.partial(join_kernel, count),
        in_specs=[pl.BlockSpec(memory_space=pltpu.MemorySpace.SMEM)]
        + [pl.BlockSpec(memory_space=VMEM)] * count,
        out_specs=[pl.BlockSpec(memory_space=VMEM)] * 2,
        out_shape=[
            jax.ShapeDtypeStruct((4, cols), jnp.float32),
            jax.ShapeDtypeStruct((max(8, count), cols), jnp.float32),
        ],
        compiler_params=pltpu.CompilerParams(vmem_limit_bytes=16 * 2**20),
        name="join",
    )(place, *parts)


def scale_kernel(index, train, low_t, high, factor, serve):
    fresh = merged(train[...], low_t[...], high[...])
    serve[...] = (fresh / factor[pl.ds(index, 1), :]).astype(serve.dtype)


def scaled(index, train, low_t, high, factor, low_at=0):
    rows, cols = train.shape
    rank = high.shape[0]
    tile = tile_of(rows)
    first = low_at // tile
    return pl.pallas_call(
        functools.partial(scale_kernel, index),
        grid=(rows // tile,),
        in_specs=[
            pl.BlockSpec((tile, cols), lambda i: (i, 0)),
            pl.BlockSpec((rank, tile), lambda i: (0, i + first)),
            pl.BlockSpec((rank, cols), lambda i: (0, 0)),
            pl.BlockSpec((4, cols), lambda i: (0, 0)),
        ],
        out_specs=pl.BlockSpec((tile, cols), lambda i: (i, 0)),
        out_shape=jax.ShapeDtypeStruct((rows, cols), jnp.bfloat16),
        compiler_params=pltpu.CompilerParams(vmem_limit_bytes=16 * 2**20),
        name="scale",
        cost_estimate=pl.CostEstimate(
            flops=2 * rows * cols * rank, bytes_accessed=4 * rows * cols, transcendentals=0
        ),
    )(train, low_t, high, factor)


def place_kernel(plan, count, near, place, *refs):
    sources, out, buffers = refs[1 : 1 + len(plan)], refs[1 + len(plan)], refs[2 + len(plan) :]
    slots, (read, written) = buffers[:-2], buffers[-2:]
    mine = place[0]
    for index, (shift, at, shard) in enumerate(plan):
        owner = mine + shift
        rows = sources[index].shape[0]
        part = tile_of(rows)

        @pl.when((owner >= 0) & (owner < count))
        def _(index=index, owner=owner, rows=rows, part=part, at=at, shard=shard):
            begins = range(0, rows, part)
            loads, stores = [], []
            if not near:
                for p, begin in enumerate(begins):
                    loads.append(
                        pltpu.make_async_copy(
                            sources[index].at[pl.ds(begin, part)],
                            slots[index].at[pl.ds(begin, part)],
                            read.at[index, p],
                        )
                    )
                    loads[-1].start()
            held = sources[index] if near else slots[index]
            for p, begin in enumerate(begins):
                start = pl.multiple_of(owner * shard + at + begin, part)
                if not near:
                    loads[p].wait()
                stores.append(
                    pltpu.make_async_copy(
                        held.at[pl.ds(begin, part)],
                        out.at[pl.ds(start, part)],
                        written.at[index, p],
                    )
                )
                stores[-1].start()
            for store in stores:
                store.wait()


def placed(place, out, count, plan, sources, near=True):
    pieces = max(source.shape[0] // tile_of(source.shape[0]) for source in sources)
    if near:
        sources = [pltpu.with_memory_space_constraint(source, VMEM) for source in sources]
    return pl.pallas_call(
        functools.partial(place_kernel, plan, count, near),
        in_specs=[pl.BlockSpec(memory_space=pltpu.MemorySpace.SMEM)]
        + [pl.BlockSpec(memory_space=HBM)]
        + [pl.BlockSpec(memory_space=VMEM if near else HBM)] * len(sources),
        out_specs=pl.BlockSpec(memory_space=HBM),
        out_shape=jax.ShapeDtypeStruct(out.shape, out.dtype),
        scratch_shapes=[
            pltpu.VMEM((8, 128) if near else source.shape, source.dtype) for source in sources
        ]
        + [pltpu.SemaphoreType.DMA((len(sources), pieces))] * 2,
        input_output_aliases={1: 0},
        compiler_params=pltpu.CompilerParams(vmem_limit_bytes=16 * 2**20),
        name="place",
        cost_estimate=pl.CostEstimate(
            flops=sum(source.size for source in sources),
            bytes_accessed=sum(4 * source.size for source in sources),
            transcendentals=0,
        ),
    )(place, out, *sources)


def own_kernel(index, place, train, low_t, high, factor, serve, out):
    del place
    fresh = merged(train[...], low_t[...], high[...])
    block = (fresh / factor[pl.ds(index, 1), :]).astype(serve.dtype)
    serve[...] = block
    out[...] = block


def own_scaled(index, place, count, train, low_t, high, factor):
    rows, cols = train.shape
    rank = high.shape[0]
    tile = tile_of(rows)
    steps = rows // tile
    return pl.pallas_call(
        functools.partial(own_kernel, index),
        grid_spec=pltpu.PrefetchScalarGridSpec(
            num_scalar_prefetch=1,
            grid=(steps,),
            in_specs=[
                pl.BlockSpec((tile, cols), lambda i, place: (i, 0)),
                pl.BlockSpec((rank, tile), lambda i, place: (0, i)),
                pl.BlockSpec((rank, cols), lambda i, place: (0, 0)),
                pl.BlockSpec((4, cols), lambda i, place: (0, 0)),
            ],
            out_specs=[
                pl.BlockSpec((tile, cols), lambda i, place: (i, 0)),
                pl.BlockSpec((tile, cols), lambda i, place: (place[0] * steps + i, 0)),
            ],
        ),
        out_shape=[
            jax.ShapeDtypeStruct((rows, cols), jnp.bfloat16),
            jax.ShapeDtypeStruct((count * rows, cols), jnp.bfloat16),
        ],
        compiler_params=pltpu.CompilerParams(vmem_limit_bytes=16 * 2**20),
        name="own",
        cost_estimate=pl.CostEstimate(
            flops=2 * rows * cols * rank, bytes_accessed=6 * rows * cols, transcendentals=0
        ),
    )(place, train, low_t, high, factor)


def per_device(count, *operands):
    return merged_for_serving(count, *operands)


def merged_for_serving(
    count,
    train_query,
    low_query,
    high_query,
    train_key,
    low_key,
    high_key,
    train_value,
    low_value,
    high_value,
    norm_train,
    norm_step,
):
    rows, cols = train_query.shape
    half = rows // 2
    place = lax.axis_index("zero").astype(jnp.int32).reshape(1)
    lows = (low_query.T, low_key.T, low_value.T)
    highs = (high_query, high_key, high_value)
    trains = (train_query, train_key, train_value)

    def left(x, hop):
        return lax.ppermute(x, "zero", [(i, i - 1) for i in range(1, count - hop + 1)])

    def right(x, hop):
        return lax.ppermute(x, "zero", [(i, i + 1) for i in range(hop - 1, count - 1)])

    def both(pair, hop):
        from_right, from_left = pair
        return left(from_right, hop), right(from_left, hop)

    raw = [both((train_query[:half],) * 2, 1)]
    norm = jnp.pad(norm_train + norm_step, (0, cols - norm_train.shape[0])).reshape(1, cols)
    tops = column_tops(trains, lows, highs, norm)
    parts = [tops]
    for s in range(1, count):
        parts.append(lax.ppermute(tops, "zero", [(i, (i + s) % count) for i in range(count)]))
    raw.append(both((train_query[half:],) * 2, 1))
    near = left(lows[0], 1), right(lows[0], 1)
    factor, norms = join_tops(place, parts)

    outs, sends = [None] * 3, [None] * 3
    for index in (1, 2, 0):
        sends[index], outs[index] = own_scaled(
            index, place, count, trains[index], lows[index], highs[index], factor
        )
    pieces = []
    for p in range(2):
        pair = []
        for got, low in zip(raw[p], near):
            pair.append(scaled(0, got, low, high_query, factor, p * half))
        pieces.append((f"q{p}", 0, p * half, tuple(pair)))
    for index, name in ((1, "k"), (2, "v")):
        pieces.append((name, index, 0, both((sends[index],) * 2, 1)))

    for hop in range(1, count):
        later = []
        for name, index, at, pair in pieces:
            if hop + 1 < count:
                later.append((name, index, at, both(pair, hop + 1)))
            outs[index] = placed(
                place,
                outs[index],
                count,
                ((hop, at, rows), (-hop, at, rows)),
                pair,
            )
        pieces = later

    size = norm_train.shape[0]
    wide = lax.all_gather(norms[:count, :size].astype(jnp.bfloat16), "width", axis=1, tiled=True)
    serve_norm = wide.reshape(-1)
    return (*outs, factor[0], factor[1], factor[2], serve_norm)


def solution(mesh):
    count = mesh.shape["zero"]
    return jax.shard_map(
        functools.partial(per_device, count),
        mesh=mesh,
        in_specs=(
            P(("unit", "zero"), "width"),
            P(("unit", "zero"), None),
            P("unit", "width"),
            P(("unit", "zero"), "width"),
            P(("unit", "zero"), None),
            P("unit", "width"),
            P(("unit", "zero"), "width"),
            P(("unit", "zero"), None),
            P("unit", "width"),
            P(("unit", "zero", "width")),
            P(("unit", "zero", "width")),
        ),
        out_specs=(
            P("unit", "width"),
            P("unit", "width"),
            P("unit", "width"),
            P(("unit", "width")),
            P(("unit", "width")),
            P(("unit", "width")),
            P("unit"),
        ),
        check_vma=False,
    )
```

```python
import functools

import jax
import jax.numpy as jnp
from jax import lax
from jax.experimental import pallas as pl
from jax.experimental.pallas import tpu as pltpu
from jax.sharding import PartitionSpec as P

mix_rate = 1.0


GRANT = 16 * 2**20

HBM = pltpu.MemorySpace.HBM
VMEM = pltpu.MemorySpace.VMEM


def tile_of(rows, most=256):
    tile = min(rows, most)
    while rows % tile:
        tile //= 2
    return tile


def merged(train, low_t, high):
    step = lax.dot_general(
        low_t, high, (((0,), (0,)), ((), ())), preferred_element_type=jnp.float32
    )
    return train.astype(jnp.float32) + mix_rate * step


def top_kernel(tq, tk, tv, lq, lk, lv, hq, hk, hv, norm, out, acc):
    step = pl.program_id(0)
    for index, (t, l, h) in enumerate(((tq, lq, hq), (tk, lk, hk), (tv, lv, hv))):
        size = jnp.abs(merged(t[...], l[...], h[...]))
        rows, cols = size.shape
        best = jnp.max(size.reshape(rows // 8, 8, cols), axis=0)

        @pl.when(step == 0)
        def _():
            acc[index] = best

        @pl.when(step > 0)
        def _():
            acc[index] = jnp.maximum(acc[index], best)

    @pl.when(step == pl.num_programs(0) - 1)
    def _():
        for index in range(3):
            out[pl.ds(index, 1), :] = jnp.max(acc[index], axis=0, keepdims=True)
        out[pl.ds(3, 1), :] = norm[...]


def column_tops(trains, lows, highs, norm):
    rows, cols = trains[0].shape
    rank = lows[0].shape[0]
    tile = tile_of(rows)
    return pl.pallas_call(
        top_kernel,
        grid=(rows // tile,),
        in_specs=[pl.BlockSpec((tile, cols), lambda i: (i, 0))] * 3
        + [pl.BlockSpec((rank, tile), lambda i: (0, i))] * 3
        + [pl.BlockSpec((rank, cols), lambda i: (0, 0))] * 3
        + [pl.BlockSpec((1, cols), lambda i: (0, 0))],
        out_specs=pl.BlockSpec((4, cols), lambda i: (0, 0)),
        out_shape=jax.ShapeDtypeStruct((4, cols), jnp.float32),
        scratch_shapes=[pltpu.VMEM((3, 8, cols), jnp.float32)],
        compiler_params=pltpu.CompilerParams(vmem_limit_bytes=GRANT),
        name="tops",
        cost_estimate=pl.CostEstimate(
            flops=3 * 2 * rows * cols * rank, bytes_accessed=6 * rows * cols, transcendentals=0
        ),
    )(*trains, *lows, *highs, norm)


def join_kernel(count, place, *refs):
    parts, (factor, norm) = refs[:count], refs[count:]
    total = parts[0][...]
    for part in parts[1:]:
        total = jnp.maximum(total, part[...])
    factor[...] = total
    for shift, part in enumerate(parts):
        owner = lax.rem(place[0] - shift + count, count)
        norm[pl.ds(owner, 1), :] = part[pl.ds(3, 1), :]


def join_tops(place, parts):
    count, cols = len(parts), parts[0].shape[1]
    return pl.pallas_call(
        functools.partial(join_kernel, count),
        in_specs=[pl.BlockSpec(memory_space=pltpu.MemorySpace.SMEM)]
        + [pl.BlockSpec(memory_space=VMEM)] * count,
        out_specs=[pl.BlockSpec(memory_space=VMEM)] * 2,
        out_shape=[
            jax.ShapeDtypeStruct((4, cols), jnp.float32),
            jax.ShapeDtypeStruct((max(8, count), cols), jnp.float32),
        ],
        compiler_params=pltpu.CompilerParams(vmem_limit_bytes=GRANT),
        name="join",
    )(place, *parts)


def scale_kernel(index, train, low_t, high, factor, serve):
    fresh = merged(train[...], low_t[...], high[...])
    serve[...] = (fresh / factor[pl.ds(index, 1), :]).astype(serve.dtype)


def scaled(index, train, low_t, high, factor, low_at=0):
    rows, cols = train.shape
    rank = high.shape[0]
    tile = tile_of(rows)
    first = low_at // tile
    return pl.pallas_call(
        functools.partial(scale_kernel, index),
        grid=(rows // tile,),
        in_specs=[
            pl.BlockSpec((tile, cols), lambda i: (i, 0)),
            pl.BlockSpec((rank, tile), lambda i: (0, i + first)),
            pl.BlockSpec((rank, cols), lambda i: (0, 0)),
            pl.BlockSpec((4, cols), lambda i: (0, 0)),
        ],
        out_specs=pl.BlockSpec((tile, cols), lambda i: (i, 0)),
        out_shape=jax.ShapeDtypeStruct((rows, cols), jnp.bfloat16),
        compiler_params=pltpu.CompilerParams(vmem_limit_bytes=GRANT),
        name="scale",
        cost_estimate=pl.CostEstimate(
            flops=2 * rows * cols * rank, bytes_accessed=4 * rows * cols, transcendentals=0
        ),
    )(train, low_t, high, factor)


def owner_of(mine, side, hop):
    return mine + hop * (1 - 2 * lax.rem(mine + side, 2))


def place_kernel(hop, sides, at, shard, count, place, *refs):
    sources, out, sems = refs[1 : 1 + len(sides)], refs[1 + len(sides)], refs[2 + len(sides)]
    for index, (side, source) in enumerate(zip(sides, sources)):
        owner = owner_of(place[0], side, hop)
        rows = source.shape[0]
        part = tile_of(rows)

        @pl.when((owner >= 0) & (owner < count))
        def _(index=index, source=source, owner=owner, rows=rows, part=part):
            stores = []
            for p, begin in enumerate(range(0, rows, part)):
                start = pl.multiple_of(owner * shard + at + begin, part)
                stores.append(
                    pltpu.make_async_copy(
                        source.at[pl.ds(begin, part)], out.at[pl.ds(start, part)], sems.at[index, p]
                    )
                )
                stores[-1].start()
            for store in stores:
                store.wait()


def placed(place, out, count, hop, at, shard, arrived):
    sides = tuple(side for side, _ in arrived)
    sources = [pltpu.with_memory_space_constraint(source, VMEM) for _, source in arrived]
    rows, size = sources[0].shape[0], sum(source.size for source in sources)
    return pl.pallas_call(
        functools.partial(place_kernel, hop, sides, at, shard, count),
        in_specs=[pl.BlockSpec(memory_space=pltpu.MemorySpace.SMEM)]
        + [pl.BlockSpec(memory_space=HBM)]
        + [pl.BlockSpec(memory_space=VMEM)] * len(sources),
        out_specs=pl.BlockSpec(memory_space=HBM),
        out_shape=jax.ShapeDtypeStruct(out.shape, out.dtype),
        scratch_shapes=[pltpu.SemaphoreType.DMA((len(sources), rows // tile_of(rows)))],
        input_output_aliases={1: 0},
        compiler_params=pltpu.CompilerParams(vmem_limit_bytes=GRANT),
        name="place",
        cost_estimate=pl.CostEstimate(flops=size, bytes_accessed=4 * size, transcendentals=0),
    )(place, out, *sources)


def own_kernel(index, first, place, train, low_t, high, factor, out, *serve):
    del place
    fresh = merged(train[...], low_t[...], high[...])
    block = (fresh / factor[pl.ds(index, 1), :]).astype(out.dtype)
    out[...] = block
    if serve:

        @pl.when(pl.program_id(0) >= first)
        def _():
            serve[0][...] = block


def own_scaled(index, place, count, train, low_t, high, factor, sent):
    rows, cols = train.shape
    rank = high.shape[0]
    tile = tile_of(rows)
    steps, first = rows // tile, sent // tile
    specs = [pl.BlockSpec((tile, cols), lambda i, place: (place[0] * steps + i, 0))]
    shapes = [jax.ShapeDtypeStruct((count * rows, cols), jnp.bfloat16)]
    if sent < rows:
        specs.append(pl.BlockSpec((tile, cols), lambda i, place: (jnp.maximum(i - first, 0), 0)))
        shapes.append(jax.ShapeDtypeStruct((rows - sent, cols), jnp.bfloat16))
    return pl.pallas_call(
        functools.partial(own_kernel, index, first),
        grid_spec=pltpu.PrefetchScalarGridSpec(
            num_scalar_prefetch=1,
            grid=(steps,),
            in_specs=[
                pl.BlockSpec((tile, cols), lambda i, place: (i, 0)),
                pl.BlockSpec((rank, tile), lambda i, place: (0, i)),
                pl.BlockSpec((rank, cols), lambda i, place: (0, 0)),
                pl.BlockSpec((4, cols), lambda i, place: (0, 0)),
            ],
            out_specs=specs,
        ),
        out_shape=shapes,
        compiler_params=pltpu.CompilerParams(vmem_limit_bytes=GRANT),
        name="own",
        cost_estimate=pl.CostEstimate(
            flops=2 * rows * cols * rank, bytes_accessed=6 * rows * cols, transcendentals=0
        ),
    )(place, train, low_t, high, factor)


def pairs_of(count, side, hop):
    pairs = []
    for i in range(count):
        to = i + 1 - 2 * ((i + side) % 2)
        owner = to + hop * (i - to)
        if 0 <= to < count and 0 <= owner < count:
            pairs.append((i, to))
    return pairs


def per_device(count, *operands):
    return merged_for_serving(count, *operands)


def merged_for_serving(
    count,
    train_query,
    low_query,
    high_query,
    train_key,
    low_key,
    high_key,
    train_value,
    low_value,
    high_value,
    norm_train,
    norm_step,
):
    rows, cols = train_query.shape
    half = rows // 2
    place = lax.axis_index("zero").astype(jnp.int32).reshape(1)
    lows = (low_query.T, low_key.T, low_value.T)
    highs = (high_query, high_key, high_value)
    trains = (train_query, train_key, train_value)

    def sent(hop, first, second):
        moved = []
        for side, x in ((0, first), (1, second)):
            pairs = pairs_of(count, side, hop)
            if pairs:
                moved.append((side, lax.ppermute(x, "zero", pairs)))
        return moved

    raw = {"q": sent(1, train_query, train_query)}
    norm = jnp.pad(norm_train + norm_step, (0, cols - norm_train.shape[0])).reshape(1, cols)
    tops = column_tops(trains, lows, highs, norm)
    parts = [tops]
    for s in range(1, count):
        parts.append(lax.ppermute(tops, "zero", [(i, (i + s) % count) for i in range(count)]))
    early = train_key[:half]
    raw["ka"] = sent(1, early, early)
    low = jnp.concatenate((lows[0], lows[1][:, :half]), axis=1)
    near = dict(sent(1, low, low))
    factor, norms = join_tops(place, parts)

    outs, serves = [None] * 3, [None] * 3
    for index, begin in ((1, half), (2, 0), (0, rows)):
        outs[index], *serves[index] = own_scaled(
            index, place, count, trains[index], lows[index], highs[index], factor, begin
        )
    pieces = []
    for name, index, low_at in (("q", 0, 0), ("ka", 1, rows)):
        arrived = []
        for side, got in raw[name]:
            arrived.append((side, scaled(index, got, near[side], highs[index], factor, low_at)))
        pieces.append((name, index, 0, arrived))
    for name, index, at in (("kb", 1, half), ("v", 2, 0)):
        pieces.append((name, index, at, sent(1, serves[index][0], serves[index][0])))

    for hop in range(1, count):
        later = []
        for name, index, at, arrived in pieces:
            if hop + 1 < count:
                brought = dict(arrived)
                later.append((name, index, at, sent(hop + 1, brought.get(1), brought.get(0))))
            outs[index] = placed(place, outs[index], count, hop, at, rows, arrived)
        pieces = later

    size = norm_train.shape[0]
    wide = lax.all_gather(norms[:count, :size].astype(jnp.bfloat16), "width", axis=1, tiled=True)
    serve_norm = wide.reshape(-1)
    return (*outs, factor[0], factor[1], factor[2], serve_norm)


def solution(mesh):
    count = mesh.shape["zero"]
    return jax.shard_map(
        functools.partial(per_device, count),
        mesh=mesh,
        in_specs=(
            P(("unit", "zero"), "width"),
            P(("unit", "zero"), None),
            P("unit", "width"),
            P(("unit", "zero"), "width"),
            P(("unit", "zero"), None),
            P("unit", "width"),
            P(("unit", "zero"), "width"),
            P(("unit", "zero"), None),
            P("unit", "width"),
            P(("unit", "zero", "width")),
            P(("unit", "zero", "width")),
        ),
        out_specs=(
            P("unit", "width"),
            P("unit", "width"),
            P("unit", "width"),
            P(("unit", "width")),
            P(("unit", "width")),
            P(("unit", "width")),
            P("unit"),
        ),
        check_vma=False,
    )
```

```python
import functools
import math

import jax
import jax.numpy as jnp
from jax import lax
from jax.experimental import pallas as pl
from jax.experimental.pallas import tpu as pltpu
from jax.sharding import PartitionSpec as P

mix_rate = 1.0


GRANT = 16 * 2**20

HBM = pltpu.MemorySpace.HBM
VMEM = pltpu.MemorySpace.VMEM


def tile_of(rows, most=256):
    tile = min(rows, most)
    while rows % tile:
        tile //= 2
    return tile


def merged(train, low_t, high):
    step = lax.dot_general(
        low_t, high, (((0,), (0,)), ((), ())), preferred_element_type=jnp.float32
    )
    return train.astype(jnp.float32) + mix_rate * step


def top_kernel(tq, tk, tv, lq, lk, lv, hq, hk, hv, norm, out, acc):
    step = pl.program_id(0)
    for index, (t, l, h) in enumerate(((tq, lq, hq), (tk, lk, hk), (tv, lv, hv))):
        size = jnp.abs(merged(t[...], l[...], h[...]))
        rows, cols = size.shape
        best = jnp.max(size.reshape(rows // 8, 8, cols), axis=0)

        @pl.when(step == 0)
        def _():
            acc[index] = best

        @pl.when(step > 0)
        def _():
            acc[index] = jnp.maximum(acc[index], best)

    @pl.when(step == pl.num_programs(0) - 1)
    def _():
        for index in range(3):
            out[pl.ds(index, 1), :] = jnp.max(acc[index], axis=0, keepdims=True)
        out[pl.ds(3, 1), :] = norm[...]


def column_tops(trains, lows, highs, norm):
    rows, cols = trains[0].shape
    rank = lows[0].shape[0]
    tile = tile_of(rows)
    return pl.pallas_call(
        top_kernel,
        grid=(rows // tile,),
        in_specs=[pl.BlockSpec((tile, cols), lambda i: (i, 0))] * 3
        + [pl.BlockSpec((rank, tile), lambda i: (0, i))] * 3
        + [pl.BlockSpec((rank, cols), lambda i: (0, 0))] * 3
        + [pl.BlockSpec((1, cols), lambda i: (0, 0))],
        out_specs=pl.BlockSpec((4, cols), lambda i: (0, 0)),
        out_shape=jax.ShapeDtypeStruct((4, cols), jnp.float32),
        scratch_shapes=[pltpu.VMEM((3, 8, cols), jnp.float32)],
        compiler_params=pltpu.CompilerParams(vmem_limit_bytes=GRANT),
        name="tops",
        cost_estimate=pl.CostEstimate(
            flops=3 * 2 * rows * cols * rank, bytes_accessed=6 * rows * cols, transcendentals=0
        ),
    )(*trains, *lows, *highs, norm)


def join_kernel(count, place, *refs):
    parts, (factor, norm) = refs[:count], refs[count:]
    total = parts[0][...]
    for part in parts[1:]:
        total = jnp.maximum(total, part[...])
    factor[...] = total
    for shift, part in enumerate(parts):
        owner = lax.rem(place[0] - shift + count, count)
        norm[pl.ds(owner, 1), :] = part[pl.ds(3, 1), :]


def join_tops(place, parts):
    count, cols = len(parts), parts[0].shape[1]
    return pl.pallas_call(
        functools.partial(join_kernel, count),
        in_specs=[pl.BlockSpec(memory_space=pltpu.MemorySpace.SMEM)]
        + [pl.BlockSpec(memory_space=VMEM)] * count,
        out_specs=[pl.BlockSpec(memory_space=VMEM)] * 2,
        out_shape=[
            jax.ShapeDtypeStruct((4, cols), jnp.float32),
            jax.ShapeDtypeStruct((max(8, count), cols), jnp.float32),
        ],
        compiler_params=pltpu.CompilerParams(vmem_limit_bytes=GRANT),
        name="join",
    )(place, *parts)


def scale_kernel(index, train, low_t, high, factor, serve):
    fresh = merged(train[...], low_t[...], high[...])
    serve[...] = (fresh / factor[pl.ds(index, 1), :]).astype(serve.dtype)


def scaled(index, train, low_t, high, factor, low_at=0):
    rows, cols = train.shape
    rank = high.shape[0]
    tile = tile_of(rows)
    first = low_at // tile
    return pl.pallas_call(
        functools.partial(scale_kernel, index),
        grid=(rows // tile,),
        in_specs=[
            pl.BlockSpec((tile, cols), lambda i: (i, 0)),
            pl.BlockSpec((rank, tile), lambda i: (0, i + first)),
            pl.BlockSpec((rank, cols), lambda i: (0, 0)),
            pl.BlockSpec((4, cols), lambda i: (0, 0)),
        ],
        out_specs=pl.BlockSpec((tile, cols), lambda i: (i, 0)),
        out_shape=jax.ShapeDtypeStruct((rows, cols), jnp.bfloat16),
        compiler_params=pltpu.CompilerParams(vmem_limit_bytes=GRANT),
        name="scale",
        cost_estimate=pl.CostEstimate(
            flops=2 * rows * cols * rank, bytes_accessed=4 * rows * cols, transcendentals=0
        ),
    )(train, low_t, high, factor)


def owner_of(mine, side, hop):
    return mine + hop * (1 - 2 * lax.rem(mine + side, 2))


def place_kernel(hop, sides, at, shard, count, place, *refs):
    sources, out, sems = refs[1 : 1 + len(sides)], refs[1 + len(sides)], refs[2 + len(sides)]
    for index, (side, source) in enumerate(zip(sides, sources)):
        owner = owner_of(place[0], side, hop)
        rows = source.shape[0]
        part = tile_of(rows)

        @pl.when((owner >= 0) & (owner < count))
        def _(index=index, source=source, owner=owner, rows=rows, part=part):
            stores = []
            for p, begin in enumerate(range(0, rows, part)):
                start = pl.multiple_of(owner * shard + at + begin, part)
                stores.append(
                    pltpu.make_async_copy(
                        source.at[pl.ds(begin, part)], out.at[pl.ds(start, part)], sems.at[index, p]
                    )
                )
                stores[-1].start()
            for store in stores:
                store.wait()


def placed(place, out, count, hop, at, shard, arrived):
    sides = tuple(side for side, _ in arrived)
    sources = [pltpu.with_memory_space_constraint(source, VMEM) for _, source in arrived]
    rows, size = sources[0].shape[0], sum(source.size for source in sources)
    return pl.pallas_call(
        functools.partial(place_kernel, hop, sides, at, shard, count),
        in_specs=[pl.BlockSpec(memory_space=pltpu.MemorySpace.SMEM)]
        + [pl.BlockSpec(memory_space=HBM)]
        + [pl.BlockSpec(memory_space=VMEM)] * len(sources),
        out_specs=pl.BlockSpec(memory_space=HBM),
        out_shape=jax.ShapeDtypeStruct(out.shape, out.dtype),
        scratch_shapes=[pltpu.SemaphoreType.DMA((len(sources), rows // tile_of(rows)))],
        input_output_aliases={1: 0},
        compiler_params=pltpu.CompilerParams(vmem_limit_bytes=GRANT),
        name="place",
        cost_estimate=pl.CostEstimate(flops=size, bytes_accessed=4 * size, transcendentals=0),
    )(place, out, *sources)


def own_kernel(index, first, place, train, low_t, high, factor, out, *serve):
    del place
    fresh = merged(train[...], low_t[...], high[...])
    block = (fresh / factor[pl.ds(index, 1), :]).astype(out.dtype)
    out[...] = block
    if serve:

        @pl.when(pl.program_id(0) >= first)
        def _():
            serve[0][...] = block


def own_scaled(index, place, count, train, low_t, high, factor, sent):
    rows, cols = train.shape
    rank = high.shape[0]
    tile = tile_of(math.gcd(rows, sent))
    steps, first = rows // tile, sent // tile
    specs = [pl.BlockSpec((tile, cols), lambda i, place: (place[0] * steps + i, 0))]
    shapes = [jax.ShapeDtypeStruct((count * rows, cols), jnp.bfloat16)]
    if sent < rows:
        specs.append(pl.BlockSpec((tile, cols), lambda i, place: (jnp.maximum(i - first, 0), 0)))
        shapes.append(jax.ShapeDtypeStruct((rows - sent, cols), jnp.bfloat16))
    return pl.pallas_call(
        functools.partial(own_kernel, index, first),
        grid_spec=pltpu.PrefetchScalarGridSpec(
            num_scalar_prefetch=1,
            grid=(steps,),
            in_specs=[
                pl.BlockSpec((tile, cols), lambda i, place: (i, 0)),
                pl.BlockSpec((rank, tile), lambda i, place: (0, i)),
                pl.BlockSpec((rank, cols), lambda i, place: (0, 0)),
                pl.BlockSpec((4, cols), lambda i, place: (0, 0)),
            ],
            out_specs=specs,
        ),
        out_shape=shapes,
        compiler_params=pltpu.CompilerParams(vmem_limit_bytes=GRANT),
        name="own",
        cost_estimate=pl.CostEstimate(
            flops=2 * rows * cols * rank, bytes_accessed=6 * rows * cols, transcendentals=0
        ),
    )(place, train, low_t, high, factor)


def pairs_of(count, side, hop):
    pairs = []
    for i in range(count):
        to = i + 1 - 2 * ((i + side) % 2)
        owner = to + hop * (i - to)
        if 0 <= to < count and 0 <= owner < count:
            pairs.append((i, to))
    return pairs


def per_device(count, *operands):
    return merged_for_serving(count, *operands)


def merged_for_serving(
    count,
    train_query,
    low_query,
    high_query,
    train_key,
    low_key,
    high_key,
    train_value,
    low_value,
    high_value,
    norm_train,
    norm_step,
):
    rows, cols = train_query.shape
    half = rows // 2
    place = lax.axis_index("zero").astype(jnp.int32).reshape(1)
    lows = (low_query.T, low_key.T, low_value.T)
    highs = (high_query, high_key, high_value)
    trains = (train_query, train_key, train_value)

    def sent(hop, first, second):
        moved = []
        for side, x in ((0, first), (1, second)):
            pairs = pairs_of(count, side, hop)
            if pairs:
                moved.append((side, lax.ppermute(x, "zero", pairs)))
        return moved

    raw = {"q": sent(1, train_query, train_query)}
    norm = jnp.pad(norm_train + norm_step, (0, cols - norm_train.shape[0])).reshape(1, cols)
    tops = column_tops(trains, lows, highs, norm)
    parts = [tops]
    for s in range(1, count):
        parts.append(lax.ppermute(tops, "zero", [(i, (i + s) % count) for i in range(count)]))
    early = train_key[:half]
    raw["ka"] = sent(1, early, early)
    low = jnp.concatenate((lows[0], lows[1][:, :half]), axis=1)
    whole = low.shape[1]
    devices = lax.axis_size("width")
    shared = whole % devices == 0
    if shared:
        part = whole // devices
        low = lax.dynamic_slice_in_dim(low, lax.axis_index("width") * part, part, axis=1)
    near = dict(sent(1, low, low))
    sides = sorted(near)
    joined = jnp.stack([near[side] for side in sides])
    if shared:
        joined = lax.all_gather(joined, "width", axis=2, tiled=True)
    near = {side: joined[index] for index, side in enumerate(sides)}
    factor, norms = join_tops(place, parts)

    outs, serves = [None] * 3, [None] * 3
    for index, begin in ((1, half), (2, 0), (0, rows)):
        outs[index], *serves[index] = own_scaled(
            index, place, count, trains[index], lows[index], highs[index], factor, begin
        )
    pieces = []
    for name, index, low_at in (("q", 0, 0), ("ka", 1, rows)):
        arrived = []
        for side, got in raw[name]:
            arrived.append((side, scaled(index, got, near[side], highs[index], factor, low_at)))
        pieces.append((name, index, 0, arrived))
    cut = rows * 3 // 4
    for name, index, at, ready in (
        ("kb", 1, half, serves[1][0]),
        ("v", 2, 0, serves[2][0][:cut]),
        ("w", 2, cut, serves[2][0][cut:]),
    ):
        pieces.append((name, index, at, sent(1, ready, ready)))

    for hop in range(1, count):
        later = []
        for name, index, at, arrived in pieces:
            if hop + 1 < count:
                brought = dict(arrived)
                later.append((name, index, at, sent(hop + 1, brought.get(1), brought.get(0))))
            outs[index] = placed(place, outs[index], count, hop, at, rows, arrived)
        pieces = later

    size = norm_train.shape[0]
    wide = lax.all_gather(norms[:count, :size].astype(jnp.bfloat16), "width", axis=1, tiled=True)
    serve_norm = wide.reshape(-1)
    return (*outs, factor[0], factor[1], factor[2], serve_norm)


def solution(mesh):
    count = mesh.shape["zero"]
    return jax.shard_map(
        functools.partial(per_device, count),
        mesh=mesh,
        in_specs=(
            P(("unit", "zero"), "width"),
            P(("unit", "zero"), None),
            P("unit", "width"),
            P(("unit", "zero"), "width"),
            P(("unit", "zero"), None),
            P("unit", "width"),
            P(("unit", "zero"), "width"),
            P(("unit", "zero"), None),
            P("unit", "width"),
            P(("unit", "zero", "width")),
            P(("unit", "zero", "width")),
        ),
        out_specs=(
            P("unit", "width"),
            P("unit", "width"),
            P("unit", "width"),
            P(("unit", "width")),
            P(("unit", "width")),
            P(("unit", "width")),
            P("unit"),
        ),
        check_vma=False,
    )
```

```python
import functools
import math

import jax
import jax.numpy as jnp
from jax import lax
from jax.experimental import pallas as pl
from jax.experimental.pallas import tpu as pltpu
from jax.sharding import PartitionSpec as P

mix_rate = 1.0


GRANT = 16 * 2**20

HBM = pltpu.MemorySpace.HBM
VMEM = pltpu.MemorySpace.VMEM


def tile_of(rows, most=256):
    tile = min(rows, most)
    while rows % tile:
        tile //= 2
    return tile


def merged(train, low_t, high):
    step = lax.dot_general(
        low_t, high, (((0,), (0,)), ((), ())), preferred_element_type=jnp.float32
    )
    return train.astype(jnp.float32) + mix_rate * step


def top_kernel(tq, tk, tv, lq, lk, lv, hq, hk, hv, norm, out, acc):
    step = pl.program_id(0)
    for index, (t, l, h) in enumerate(((tq, lq, hq), (tk, lk, hk), (tv, lv, hv))):
        size = jnp.abs(merged(t[...], l[...], h[...]))
        rows, cols = size.shape
        best = jnp.max(size.reshape(rows // 8, 8, cols), axis=0)

        @pl.when(step == 0)
        def _():
            acc[index] = best

        @pl.when(step > 0)
        def _():
            acc[index] = jnp.maximum(acc[index], best)

    @pl.when(step == pl.num_programs(0) - 1)
    def _():
        for index in range(3):
            out[pl.ds(index, 1), :] = jnp.max(acc[index], axis=0, keepdims=True)
        out[pl.ds(3, 1), :] = norm[...]


def column_tops(trains, lows, highs, norm):
    rows, cols = trains[0].shape
    rank = lows[0].shape[0]
    tile = tile_of(rows)
    return pl.pallas_call(
        top_kernel,
        grid=(rows // tile,),
        in_specs=[pl.BlockSpec((tile, cols), lambda i: (i, 0))] * 3
        + [pl.BlockSpec((rank, tile), lambda i: (0, i))] * 3
        + [pl.BlockSpec((rank, cols), lambda i: (0, 0))] * 3
        + [pl.BlockSpec((1, cols), lambda i: (0, 0))],
        out_specs=pl.BlockSpec((4, cols), lambda i: (0, 0)),
        out_shape=jax.ShapeDtypeStruct((4, cols), jnp.float32),
        scratch_shapes=[pltpu.VMEM((3, 8, cols), jnp.float32)],
        compiler_params=pltpu.CompilerParams(vmem_limit_bytes=GRANT),
        name="tops",
        cost_estimate=pl.CostEstimate(
            flops=3 * 2 * rows * cols * rank, bytes_accessed=6 * rows * cols, transcendentals=0
        ),
    )(*trains, *lows, *highs, norm)


def join_kernel(count, place, *refs):
    parts, (factor, norm) = refs[:count], refs[count:]
    total = parts[0][...]
    for part in parts[1:]:
        total = jnp.maximum(total, part[...])
    factor[...] = total
    for shift, part in enumerate(parts):
        owner = lax.rem(place[0] - shift + count, count)
        norm[pl.ds(owner, 1), :] = part[pl.ds(3, 1), :]


def join_tops(place, parts):
    count, cols = len(parts), parts[0].shape[1]
    return pl.pallas_call(
        functools.partial(join_kernel, count),
        in_specs=[pl.BlockSpec(memory_space=pltpu.MemorySpace.SMEM)]
        + [pl.BlockSpec(memory_space=VMEM)] * count,
        out_specs=[pl.BlockSpec(memory_space=VMEM)] * 2,
        out_shape=[
            jax.ShapeDtypeStruct((4, cols), jnp.float32),
            jax.ShapeDtypeStruct((max(8, count), cols), jnp.float32),
        ],
        compiler_params=pltpu.CompilerParams(vmem_limit_bytes=GRANT),
        name="join",
    )(place, *parts)


def scale_kernel(index, train, low_t, high, factor, serve):
    fresh = merged(train[...], low_t[...], high[...])
    serve[...] = (fresh / factor[pl.ds(index, 1), :]).astype(serve.dtype)


def scaled(index, train, low_t, high, factor, low_at=0):
    rows, cols = train.shape
    rank = high.shape[0]
    tile = tile_of(rows)
    first = low_at // tile
    return pl.pallas_call(
        functools.partial(scale_kernel, index),
        grid=(rows // tile,),
        in_specs=[
            pl.BlockSpec((tile, cols), lambda i: (i, 0)),
            pl.BlockSpec((rank, tile), lambda i: (0, i + first)),
            pl.BlockSpec((rank, cols), lambda i: (0, 0)),
            pl.BlockSpec((4, cols), lambda i: (0, 0)),
        ],
        out_specs=pl.BlockSpec((tile, cols), lambda i: (i, 0)),
        out_shape=jax.ShapeDtypeStruct((rows, cols), jnp.bfloat16),
        compiler_params=pltpu.CompilerParams(vmem_limit_bytes=GRANT),
        name="scale",
        cost_estimate=pl.CostEstimate(
            flops=2 * rows * cols * rank, bytes_accessed=4 * rows * cols, transcendentals=0
        ),
    )(train, low_t, high, factor)


def owner_of(mine, side, hop):
    return mine + hop * (1 - 2 * lax.rem(mine + side, 2))


def place_kernel(hop, sides, at, shard, count, *refs):
    sources, out, sems = refs[1 : 1 + len(sides)], refs[1 + len(sides)], refs[2 + len(sides)]
    for index, (side, source) in enumerate(zip(sides, sources)):
        owner = owner_of(lax.axis_index("zero").astype(jnp.int32), side, hop)
        rows = source.shape[0]
        part = tile_of(rows)

        @pl.when((owner >= 0) & (owner < count))
        def _(index=index, source=source, owner=owner, rows=rows, part=part):
            stores = []
            for p, begin in enumerate(range(0, rows, part)):
                start = pl.multiple_of(owner * shard + at + begin, part)
                stores.append(
                    pltpu.make_async_copy(
                        source.at[pl.ds(begin, part)], out.at[pl.ds(start, part)], sems.at[index, p]
                    )
                )
                stores[-1].start()
            for store in stores:
                store.wait()


def placed(out, count, hop, at, shard, arrived):
    sides = tuple(side for side, _ in arrived)
    sources = [pltpu.with_memory_space_constraint(source, VMEM) for _, source in arrived]
    rows, size = sources[0].shape[0], sum(source.size for source in sources)
    return pl.pallas_call(
        functools.partial(place_kernel, hop, sides, at, shard, count),
        in_specs=[pl.BlockSpec(memory_space=HBM)]
        + [pl.BlockSpec(memory_space=VMEM)] * len(sources),
        out_specs=pl.BlockSpec(memory_space=HBM),
        out_shape=jax.ShapeDtypeStruct(out.shape, out.dtype),
        scratch_shapes=[pltpu.SemaphoreType.DMA((len(sources), rows // tile_of(rows)))],
        input_output_aliases={0: 0},
        compiler_params=pltpu.CompilerParams(vmem_limit_bytes=GRANT),
        name="place",
        cost_estimate=pl.CostEstimate(flops=size, bytes_accessed=4 * size, transcendentals=0),
    )(out, *sources)


def own_kernel(index, first, place, train, low_t, high, factor, out, *serve):
    del place
    fresh = merged(train[...], low_t[...], high[...])
    block = (fresh / factor[pl.ds(index, 1), :]).astype(out.dtype)
    out[...] = block
    if serve:

        @pl.when(pl.program_id(0) >= first)
        def _():
            serve[0][...] = block


def own_scaled(index, place, count, train, low_t, high, factor, sent):
    rows, cols = train.shape
    rank = high.shape[0]
    tile = tile_of(math.gcd(rows, sent))
    steps, first = rows // tile, sent // tile
    specs = [pl.BlockSpec((tile, cols), lambda i, place: (place[0] * steps + i, 0))]
    shapes = [jax.ShapeDtypeStruct((count * rows, cols), jnp.bfloat16)]
    if sent < rows:
        specs.append(pl.BlockSpec((tile, cols), lambda i, place: (jnp.maximum(i - first, 0), 0)))
        shapes.append(jax.ShapeDtypeStruct((rows - sent, cols), jnp.bfloat16))
    return pl.pallas_call(
        functools.partial(own_kernel, index, first),
        grid_spec=pltpu.PrefetchScalarGridSpec(
            num_scalar_prefetch=1,
            grid=(steps,),
            in_specs=[
                pl.BlockSpec((tile, cols), lambda i, place: (i, 0)),
                pl.BlockSpec((rank, tile), lambda i, place: (0, i)),
                pl.BlockSpec((rank, cols), lambda i, place: (0, 0)),
                pl.BlockSpec((4, cols), lambda i, place: (0, 0)),
            ],
            out_specs=specs,
        ),
        out_shape=shapes,
        compiler_params=pltpu.CompilerParams(vmem_limit_bytes=GRANT),
        name="own",
        cost_estimate=pl.CostEstimate(
            flops=2 * rows * cols * rank, bytes_accessed=6 * rows * cols, transcendentals=0
        ),
    )(place, train, low_t, high, factor)


def pairs_of(count, side, hop):
    pairs = []
    for i in range(count):
        to = i + 1 - 2 * ((i + side) % 2)
        owner = to + hop * (i - to)
        if 0 <= to < count and 0 <= owner < count:
            pairs.append((i, to))
    return pairs


def per_device(count, *operands):
    return merged_for_serving(count, *operands)


def merged_for_serving(
    count,
    train_query,
    low_query,
    high_query,
    train_key,
    low_key,
    high_key,
    train_value,
    low_value,
    high_value,
    norm_train,
    norm_step,
):
    rows, cols = train_query.shape
    half = rows // 2
    place = lax.axis_index("zero").astype(jnp.int32).reshape(1)
    lows = (low_query.T, low_key.T, low_value.T)
    highs = (high_query, high_key, high_value)
    trains = (train_query, train_key, train_value)

    def sent(hop, first, second):
        moved = []
        for side, x in ((0, first), (1, second)):
            pairs = pairs_of(count, side, hop)
            if pairs:
                moved.append((side, lax.ppermute(x, "zero", pairs)))
        return moved

    raw = {"q": sent(1, train_query, train_query)}
    norm = jnp.pad(norm_train + norm_step, (0, cols - norm_train.shape[0])).reshape(1, cols)
    tops = column_tops(trains, lows, highs, norm)
    parts = [tops]
    for s in range(1, count):
        pairs = [(i, (i + s) % count) for i in range(count) if (i + s) % count]
        parts.append(lax.ppermute(tops, "zero", pairs))
    raw["ka"] = sent(1, train_key[:half], train_key[:half])
    low = jnp.concatenate((lows[0], lows[1]), axis=1)
    whole = low.shape[1]
    devices = lax.axis_size("width")
    shared = whole % devices == 0
    if shared:
        part = whole // devices
        low = lax.dynamic_slice_in_dim(low, lax.axis_index("width") * part, part, axis=1)
    near = dict(sent(1, low, low))
    sides = sorted(near)
    joined = jnp.stack([near[side] for side in sides])
    if shared:
        joined = lax.all_gather(joined, "width", axis=2, tiled=True)
    near = {side: joined[index] for index, side in enumerate(sides)}
    joined_tops, norms = join_tops(place, parts)
    factor = jnp.maximum(joined_tops, lax.ppermute(joined_tops, "zero", [(1, 0)]))
    raw["kb"] = sent(1, train_key[half:], train_key[half:])

    outs, serves = [None] * 3, [None] * 3
    for index, begin in ((2, 0), (1, rows), (0, rows)):
        outs[index], *serves[index] = own_scaled(
            index, place, count, trains[index], lows[index], highs[index], factor, begin
        )
    pieces = []
    for name, index, at, low_at in (("q", 0, 0, 0), ("ka", 1, 0, rows), ("kb", 1, half, rows + half)):
        arrived = []
        for side, got in raw[name]:
            arrived.append((side, scaled(index, got, near[side], highs[index], factor, low_at)))
        pieces.append((name, index, at, arrived))
    cut = rows * 3 // 4
    for name, index, at, ready in (
        ("v", 2, 0, serves[2][0][:cut]),
        ("w", 2, cut, serves[2][0][cut:]),
    ):
        pieces.append((name, index, at, sent(1, ready, ready)))

    for hop in range(1, count):
        later = []
        for name, index, at, arrived in pieces:
            if hop + 1 < count:
                brought = dict(arrived)
                later.append((name, index, at, sent(hop + 1, brought.get(1), brought.get(0))))
            outs[index] = placed(outs[index], count, hop, at, rows, arrived)
        pieces = later

    size = norm_train.shape[0]
    narrow = norms[:count, :size].astype(jnp.bfloat16)
    moved = lax.ppermute(narrow, "zero", [(1, 0)])
    narrow = jnp.where(place == 0, moved, narrow)
    wide = lax.all_gather(narrow, "width", axis=1, tiled=True)
    serve_norm = wide.reshape(-1)
    return (*outs, factor[0], factor[1], factor[2], serve_norm)


def solution(mesh):
    count = mesh.shape["zero"]
    return jax.shard_map(
        functools.partial(per_device, count),
        mesh=mesh,
        in_specs=(
            P(("unit", "zero"), "width"),
            P(("unit", "zero"), None),
            P("unit", "width"),
            P(("unit", "zero"), "width"),
            P(("unit", "zero"), None),
            P("unit", "width"),
            P(("unit", "zero"), "width"),
            P(("unit", "zero"), None),
            P("unit", "width"),
            P(("unit", "zero", "width")),
            P(("unit", "zero", "width")),
        ),
        out_specs=(
            P("unit", "width"),
            P("unit", "width"),
            P("unit", "width"),
            P(("unit", "width")),
            P(("unit", "width")),
            P(("unit", "width")),
            P("unit"),
        ),
        check_vma=False,
    )
```

```python
import functools
import math

import jax
import jax.numpy as jnp
from jax import lax
from jax.experimental import pallas as pl
from jax.experimental.pallas import tpu as pltpu
from jax.sharding import PartitionSpec as P

mix_rate = 1.0


GRANT = 16 * 2**20

HBM = pltpu.MemorySpace.HBM
VMEM = pltpu.MemorySpace.VMEM


def tile_of(rows, most=256):
    tile = min(rows, most)
    while rows % tile:
        tile //= 2
    return tile


def merged(train, low_t, high):
    step = lax.dot_general(
        low_t, high, (((0,), (0,)), ((), ())), preferred_element_type=jnp.float32
    )
    return train.astype(jnp.float32) + mix_rate * step


def top_kernel(tq, tk, tv, lq, lk, lv, hq, hk, hv, norm, out, acc):
    step = pl.program_id(0)
    for index, (t, l, h) in enumerate(((tq, lq, hq), (tk, lk, hk), (tv, lv, hv))):
        size = jnp.abs(merged(t[...], l[...], h[...]))
        rows, cols = size.shape
        best = jnp.max(size.reshape(rows // 8, 8, cols), axis=0)

        @pl.when(step == 0)
        def _():
            acc[index] = best

        @pl.when(step > 0)
        def _():
            acc[index] = jnp.maximum(acc[index], best)

    @pl.when(step == pl.num_programs(0) - 1)
    def _():
        for index in range(3):
            out[pl.ds(index, 1), :] = jnp.max(acc[index], axis=0, keepdims=True)
        out[pl.ds(3, 1), :] = norm[...]


def column_tops(trains, lows, highs, norm):
    rows, cols = trains[0].shape
    rank = lows[0].shape[0]
    tile = tile_of(rows)
    return pl.pallas_call(
        top_kernel,
        grid=(rows // tile,),
        in_specs=[pl.BlockSpec((tile, cols), lambda i: (i, 0))] * 3
        + [pl.BlockSpec((rank, tile), lambda i: (0, i))] * 3
        + [pl.BlockSpec((rank, cols), lambda i: (0, 0))] * 3
        + [pl.BlockSpec((1, cols), lambda i: (0, 0))],
        out_specs=pl.BlockSpec((4, cols), lambda i: (0, 0)),
        out_shape=jax.ShapeDtypeStruct((4, cols), jnp.float32),
        scratch_shapes=[pltpu.VMEM((3, 8, cols), jnp.float32)],
        name="tops",
        cost_estimate=pl.CostEstimate(
            flops=3 * 2 * rows * cols * rank, bytes_accessed=6 * rows * cols, transcendentals=0
        ),
    )(*trains, *lows, *highs, norm)


def join_kernel(count, place, *refs):
    parts, (factor, norm) = refs[:count], refs[count:]
    total = parts[0][...]
    for part in parts[1:]:
        total = jnp.maximum(total, part[...])
    factor[...] = total
    for shift, part in enumerate(parts):
        owner = lax.rem(place[0] - shift + count, count)
        norm[pl.ds(owner, 1), :] = part[pl.ds(3, 1), :]


def join_tops(place, parts):
    count, cols = len(parts), parts[0].shape[1]
    return pl.pallas_call(
        functools.partial(join_kernel, count),
        in_specs=[pl.BlockSpec(memory_space=pltpu.MemorySpace.SMEM)]
        + [pl.BlockSpec(memory_space=VMEM)] * count,
        out_specs=[pl.BlockSpec(memory_space=VMEM)] * 2,
        out_shape=[
            jax.ShapeDtypeStruct((4, cols), jnp.float32),
            jax.ShapeDtypeStruct((max(8, count), cols), jnp.float32),
        ],
        compiler_params=pltpu.CompilerParams(vmem_limit_bytes=GRANT),
        name="join",
    )(place, *parts)


def scale_kernel(index, train, low_t, high, factor, serve):
    fresh = merged(train[...], low_t[...], high[...])
    serve[...] = (fresh / factor[pl.ds(index, 1), :]).astype(serve.dtype)


def scaled(index, train, low_t, high, factor, low_at=0):
    rows, cols = train.shape
    rank = high.shape[0]
    tile = tile_of(rows)
    first = low_at // tile
    return pl.pallas_call(
        functools.partial(scale_kernel, index),
        grid=(rows // tile,),
        in_specs=[
            pl.BlockSpec((tile, cols), lambda i: (i, 0)),
            pl.BlockSpec((rank, tile), lambda i: (0, i + first)),
            pl.BlockSpec((rank, cols), lambda i: (0, 0)),
            pl.BlockSpec((4, cols), lambda i: (0, 0)),
        ],
        out_specs=pl.BlockSpec((tile, cols), lambda i: (i, 0)),
        out_shape=jax.ShapeDtypeStruct((rows, cols), jnp.bfloat16),
        compiler_params=pltpu.CompilerParams(vmem_limit_bytes=GRANT),
        name="scale",
        cost_estimate=pl.CostEstimate(
            flops=2 * rows * cols * rank, bytes_accessed=4 * rows * cols, transcendentals=0
        ),
    )(train, low_t, high, factor)


def owner_of(mine, side, hop):
    return mine + hop * (1 - 2 * lax.rem(mine + side, 2))


def place_kernel(hop, sides, at, shard, count, *refs):
    sources, out, sems = refs[1 : 1 + len(sides)], refs[1 + len(sides)], refs[2 + len(sides)]
    for index, (side, source) in enumerate(zip(sides, sources)):
        owner = owner_of(lax.axis_index("zero").astype(jnp.int32), side, hop)
        rows = source.shape[0]
        part = tile_of(rows)

        @pl.when((owner >= 0) & (owner < count))
        def _(index=index, source=source, owner=owner, rows=rows, part=part):
            stores = []
            for p, begin in enumerate(range(0, rows, part)):
                start = pl.multiple_of(owner * shard + at + begin, part)
                stores.append(
                    pltpu.make_async_copy(
                        source.at[pl.ds(begin, part)], out.at[pl.ds(start, part)], sems.at[index, p]
                    )
                )
                stores[-1].start()
            for store in stores:
                store.wait()


def placed(out, count, hop, at, shard, arrived):
    sides = tuple(side for side, _ in arrived)
    sources = [pltpu.with_memory_space_constraint(source, VMEM) for _, source in arrived]
    rows, size = sources[0].shape[0], sum(source.size for source in sources)
    return pl.pallas_call(
        functools.partial(place_kernel, hop, sides, at, shard, count),
        in_specs=[pl.BlockSpec(memory_space=HBM)]
        + [pl.BlockSpec(memory_space=VMEM)] * len(sources),
        out_specs=pl.BlockSpec(memory_space=HBM),
        out_shape=jax.ShapeDtypeStruct(out.shape, out.dtype),
        scratch_shapes=[pltpu.SemaphoreType.DMA((len(sources), rows // tile_of(rows)))],
        input_output_aliases={0: 0},
        compiler_params=pltpu.CompilerParams(vmem_limit_bytes=GRANT),
        name="place",
        cost_estimate=pl.CostEstimate(flops=size, bytes_accessed=4 * size, transcendentals=0),
    )(out, *sources)


def own_kernel(index, first, place, train, low_t, high, factor, out, *serve):
    del place
    fresh = merged(train[...], low_t[...], high[...])
    block = (fresh / factor[pl.ds(index, 1), :]).astype(out.dtype)
    out[...] = block
    if serve:

        @pl.when(pl.program_id(0) >= first)
        def _():
            serve[0][...] = block


def own_scaled(index, place, count, train, low_t, high, factor, sent):
    rows, cols = train.shape
    rank = high.shape[0]
    tile = tile_of(math.gcd(rows, sent))
    steps, first = rows // tile, sent // tile
    specs = [pl.BlockSpec((tile, cols), lambda i, place: (place[0] * steps + i, 0))]
    shapes = [jax.ShapeDtypeStruct((count * rows, cols), jnp.bfloat16)]
    if sent < rows:
        specs.append(pl.BlockSpec((tile, cols), lambda i, place: (jnp.maximum(i - first, 0), 0)))
        shapes.append(jax.ShapeDtypeStruct((rows - sent, cols), jnp.bfloat16))
    return pl.pallas_call(
        functools.partial(own_kernel, index, first),
        grid_spec=pltpu.PrefetchScalarGridSpec(
            num_scalar_prefetch=1,
            grid=(steps,),
            in_specs=[
                pl.BlockSpec((tile, cols), lambda i, place: (i, 0)),
                pl.BlockSpec((rank, tile), lambda i, place: (0, i)),
                pl.BlockSpec((rank, cols), lambda i, place: (0, 0)),
                pl.BlockSpec((4, cols), lambda i, place: (0, 0)),
            ],
            out_specs=specs,
        ),
        out_shape=shapes,
        compiler_params=pltpu.CompilerParams(vmem_limit_bytes=GRANT),
        name="own",
        cost_estimate=pl.CostEstimate(
            flops=2 * rows * cols * rank, bytes_accessed=6 * rows * cols, transcendentals=0
        ),
    )(place, train, low_t, high, factor)


def pairs_of(count, side, hop):
    pairs = []
    for i in range(count):
        to = i + 1 - 2 * ((i + side) % 2)
        owner = to + hop * (i - to)
        if 0 <= to < count and 0 <= owner < count:
            pairs.append((i, to))
    return pairs


def per_device(count, *operands):
    return merged_for_serving(count, *operands)


def merged_for_serving(
    count,
    train_query,
    low_query,
    high_query,
    train_key,
    low_key,
    high_key,
    train_value,
    low_value,
    high_value,
    norm_train,
    norm_step,
):
    rows, cols = train_query.shape
    half = rows // 2
    place = lax.axis_index("zero").astype(jnp.int32).reshape(1)
    lows = (low_query.T, low_key.T, low_value.T)
    highs = (high_query, high_key, high_value)
    trains = (train_query, train_key, train_value)

    def sent(hop, first, second):
        moved = []
        for side, x in ((0, first), (1, second)):
            pairs = pairs_of(count, side, hop)
            if pairs:
                moved.append((side, lax.ppermute(x, "zero", pairs)))
        return moved

    raw = {"q": sent(1, train_query, train_query)}
    norm = jnp.pad(norm_train + norm_step, (0, cols - norm_train.shape[0])).reshape(1, cols)
    tops = column_tops(trains, lows, highs, norm)
    ends = {0: 1, count - 1: count - 2} if count > 2 else {0: 1}
    back = [(neighbour, end) for end, neighbour in ends.items()]
    parts = [tops]
    for s in range(1, count):
        pairs = [(i, (i + s) % count) for i in range(count) if (i + s) % count not in ends]
        parts.append(lax.ppermute(tops, "zero", pairs))
    raw["ka"] = sent(1, train_key[:half], train_key[:half])
    low = jnp.concatenate((lows[0], lows[1]), axis=1)
    whole = low.shape[1]
    devices = lax.axis_size("width")
    shared = whole % devices == 0
    if shared:
        part = whole // devices
        low = lax.dynamic_slice_in_dim(low, lax.axis_index("width") * part, part, axis=1)
    near = dict(sent(1, low, low))
    sides = sorted(near)
    joined = jnp.stack([near[side] for side in sides])
    if shared:
        joined = lax.all_gather(joined, "width", axis=2, tiled=True)
    near = {side: joined[index] for index, side in enumerate(sides)}
    joined_tops, norms = join_tops(place, parts)
    factor = jnp.maximum(joined_tops, lax.ppermute(joined_tops, "zero", back))
    raw["kb"] = sent(1, train_key[half:], train_key[half:])

    outs, serves = [None] * 3, [None] * 3
    for index, begin in ((2, 0), (1, rows), (0, rows)):
        outs[index], *serves[index] = own_scaled(
            index, place, count, trains[index], lows[index], highs[index], factor, begin
        )
    pieces = []
    for name, index, at, low_at in (("q", 0, 0, 0), ("ka", 1, 0, rows), ("kb", 1, half, rows + half)):
        arrived = []
        for side, got in raw[name]:
            arrived.append((side, scaled(index, got, near[side], highs[index], factor, low_at)))
        pieces.append((name, index, at, arrived))
    cut = rows * 3 // 4
    for name, index, at, ready in (
        ("v", 2, 0, serves[2][0][:cut]),
        ("w", 2, cut, serves[2][0][cut:]),
    ):
        pieces.append((name, index, at, sent(1, ready, ready)))

    for hop in range(1, count):
        later = []
        for name, index, at, arrived in pieces:
            if hop + 1 < count:
                brought = dict(arrived)
                later.append((name, index, at, sent(hop + 1, brought.get(1), brought.get(0))))
            outs[index] = placed(outs[index], count, hop, at, rows, arrived)
        pieces = later

    size = norm_train.shape[0]
    narrow = norms[:count, :size].astype(jnp.bfloat16)
    moved = lax.ppermute(narrow, "zero", back)
    at_end = functools.reduce(jnp.logical_or, [place == end for end in ends])
    narrow = jnp.where(at_end, moved, narrow)
    wide = lax.all_gather(narrow, "width", axis=1, tiled=True)
    serve_norm = wide.reshape(-1)
    return (*outs, factor[0], factor[1], factor[2], serve_norm)


def solution(mesh):
    count = mesh.shape["zero"]
    return jax.shard_map(
        functools.partial(per_device, count),
        mesh=mesh,
        in_specs=(
            P(("unit", "zero"), "width"),
            P(("unit", "zero"), None),
            P("unit", "width"),
            P(("unit", "zero"), "width"),
            P(("unit", "zero"), None),
            P("unit", "width"),
            P(("unit", "zero"), "width"),
            P(("unit", "zero"), None),
            P("unit", "width"),
            P(("unit", "zero", "width")),
            P(("unit", "zero", "width")),
        ),
        out_specs=(
            P("unit", "width"),
            P("unit", "width"),
            P("unit", "width"),
            P(("unit", "width")),
            P(("unit", "width")),
            P(("unit", "width")),
            P("unit"),
        ),
        check_vma=False,
    )
```

```python
import functools
import math

import jax
import jax.numpy as jnp
from jax import lax
from jax.experimental import pallas as pl
from jax.experimental.pallas import tpu as pltpu
from jax.sharding import PartitionSpec as P

mix_rate = 1.0


GRANT = 16 * 2**20

HBM = pltpu.MemorySpace.HBM
VMEM = pltpu.MemorySpace.VMEM


def tile_of(rows, most=256):
    tile = min(rows, most)
    while rows % tile:
        tile //= 2
    return tile


def merged(train, low_t, high):
    step = lax.dot_general(
        low_t, high, (((0,), (0,)), ((), ())), preferred_element_type=jnp.float32
    )
    return train.astype(jnp.float32) + mix_rate * step


def top_kernel(tq, tk, tv, lq, lk, lv, hq, hk, hv, trained, moved, out, acc):
    step = pl.program_id(0)
    for index, (t, l, h) in enumerate(((tq, lq, hq), (tk, lk, hk), (tv, lv, hv))):
        size = jnp.abs(merged(t[...], l[...], h[...]))
        rows, cols = size.shape
        best = jnp.max(size.reshape(rows // 8, 8, cols), axis=0)

        @pl.when(step == 0)
        def _():
            acc[index] = best

        @pl.when(step > 0)
        def _():
            acc[index] = jnp.maximum(acc[index], best)

    @pl.when(step == pl.num_programs(0) - 1)
    def _():
        for index in range(3):
            out[pl.ds(index, 1), :] = jnp.max(acc[index], axis=0, keepdims=True)
        out[pl.ds(3, 1), :] = jnp.zeros((1, out.shape[1]), jnp.float32)
        out[pl.ds(3, 1), pl.ds(0, trained.shape[1])] = trained[...] + moved[...]


def column_tops(trains, lows, highs, norms):
    rows, cols = trains[0].shape
    rank = lows[0].shape[0]
    tile = tile_of(rows)
    return pl.pallas_call(
        top_kernel,
        grid=(rows // tile,),
        in_specs=[pl.BlockSpec((tile, cols), lambda i: (i, 0))] * 3
        + [pl.BlockSpec((rank, tile), lambda i: (0, i))] * 3
        + [pl.BlockSpec((rank, cols), lambda i: (0, 0))] * 3
        + [pl.BlockSpec(norms[0].shape, lambda i: (0, 0))] * 2,
        out_specs=pl.BlockSpec((4, cols), lambda i: (0, 0)),
        out_shape=jax.ShapeDtypeStruct((4, cols), jnp.float32),
        scratch_shapes=[pltpu.VMEM((3, 8, cols), jnp.float32)],
        name="tops",
        cost_estimate=pl.CostEstimate(
            flops=3 * 2 * rows * cols * rank, bytes_accessed=6 * rows * cols, transcendentals=0
        ),
    )(*trains, *lows, *highs, *norms)


def join_kernel(count, place, *refs):
    parts, (factor, norm) = refs[:count], refs[count:]
    total = parts[0][...]
    for part in parts[1:]:
        total = jnp.maximum(total, part[...])
    factor[...] = total
    for shift, part in enumerate(parts):
        owner = lax.rem(place[0] - shift + count, count)
        norm[pl.ds(owner, 1), :] = part[pl.ds(3, 1), :]


def join_tops(place, parts):
    count, cols = len(parts), parts[0].shape[1]
    return pl.pallas_call(
        functools.partial(join_kernel, count),
        in_specs=[pl.BlockSpec(memory_space=pltpu.MemorySpace.SMEM)]
        + [pl.BlockSpec(memory_space=VMEM)] * count,
        out_specs=[pl.BlockSpec(memory_space=VMEM)] * 2,
        out_shape=[
            jax.ShapeDtypeStruct((4, cols), jnp.float32),
            jax.ShapeDtypeStruct((max(8, count), cols), jnp.float32),
        ],
        compiler_params=pltpu.CompilerParams(vmem_limit_bytes=GRANT),
        name="join",
    )(place, *parts)


def scale_kernel(index, train, low_t, high, factor, serve):
    fresh = merged(train[...], low_t[...], high[...])
    serve[...] = (fresh / factor[pl.ds(index, 1), :]).astype(serve.dtype)


def scaled(index, train, low_t, high, factor, low_at=0):
    rows, cols = train.shape
    rank = high.shape[0]
    tile = tile_of(rows)
    first = low_at // tile
    return pl.pallas_call(
        functools.partial(scale_kernel, index),
        grid=(rows // tile,),
        in_specs=[
            pl.BlockSpec((tile, cols), lambda i: (i, 0)),
            pl.BlockSpec((rank, tile), lambda i: (0, i + first)),
            pl.BlockSpec((rank, cols), lambda i: (0, 0)),
            pl.BlockSpec((4, cols), lambda i: (0, 0)),
        ],
        out_specs=pl.BlockSpec((tile, cols), lambda i: (i, 0)),
        out_shape=jax.ShapeDtypeStruct((rows, cols), jnp.bfloat16),
        compiler_params=pltpu.CompilerParams(vmem_limit_bytes=GRANT),
        name="scale",
        cost_estimate=pl.CostEstimate(
            flops=2 * rows * cols * rank, bytes_accessed=4 * rows * cols, transcendentals=0
        ),
    )(train, low_t, high, factor)


def owner_of(mine, side, hop):
    return mine + hop * (1 - 2 * lax.rem(mine + side, 2))


def place_kernel(hop, sides, at, shard, count, *refs):
    sources, out, sems = refs[1 : 1 + len(sides)], refs[1 + len(sides)], refs[2 + len(sides)]
    for index, (side, source) in enumerate(zip(sides, sources)):
        owner = owner_of(lax.axis_index("zero").astype(jnp.int32), side, hop)
        rows = source.shape[0]
        part = tile_of(rows)

        @pl.when((owner >= 0) & (owner < count))
        def _(index=index, source=source, owner=owner, rows=rows, part=part):
            stores = []
            for p, begin in enumerate(range(0, rows, part)):
                start = pl.multiple_of(owner * shard + at + begin, part)
                stores.append(
                    pltpu.make_async_copy(
                        source.at[pl.ds(begin, part)], out.at[pl.ds(start, part)], sems.at[index, p]
                    )
                )
                stores[-1].start()
            for store in stores:
                store.wait()


def placed(out, count, hop, at, shard, arrived):
    sides = tuple(side for side, _ in arrived)
    sources = [pltpu.with_memory_space_constraint(source, VMEM) for _, source in arrived]
    rows, size = sources[0].shape[0], sum(source.size for source in sources)
    return pl.pallas_call(
        functools.partial(place_kernel, hop, sides, at, shard, count),
        in_specs=[pl.BlockSpec(memory_space=HBM)]
        + [pl.BlockSpec(memory_space=VMEM)] * len(sources),
        out_specs=pl.BlockSpec(memory_space=HBM),
        out_shape=jax.ShapeDtypeStruct(out.shape, out.dtype),
        scratch_shapes=[pltpu.SemaphoreType.DMA((len(sources), rows // tile_of(rows)))],
        input_output_aliases={0: 0},
        compiler_params=pltpu.CompilerParams(vmem_limit_bytes=GRANT),
        name="place",
        cost_estimate=pl.CostEstimate(flops=size, bytes_accessed=4 * size, transcendentals=0),
    )(out, *sources)


def own_kernel(index, first, place, train, low_t, high, factor, out, *serve):
    del place
    fresh = merged(train[...], low_t[...], high[...])
    block = (fresh / factor[pl.ds(index, 1), :]).astype(out.dtype)
    out[...] = block
    if serve:

        @pl.when(pl.program_id(0) >= first)
        def _():
            serve[0][...] = block


def own_scaled(index, place, count, train, low_t, high, factor, sent):
    rows, cols = train.shape
    rank = high.shape[0]
    tile = tile_of(math.gcd(rows, sent))
    steps, first = rows // tile, sent // tile
    specs = [pl.BlockSpec((tile, cols), lambda i, place: (place[0] * steps + i, 0))]
    shapes = [jax.ShapeDtypeStruct((count * rows, cols), jnp.bfloat16)]
    if sent < rows:
        specs.append(pl.BlockSpec((tile, cols), lambda i, place: (jnp.maximum(i - first, 0), 0)))
        shapes.append(jax.ShapeDtypeStruct((rows - sent, cols), jnp.bfloat16))
    return pl.pallas_call(
        functools.partial(own_kernel, index, first),
        grid_spec=pltpu.PrefetchScalarGridSpec(
            num_scalar_prefetch=1,
            grid=(steps,),
            in_specs=[
                pl.BlockSpec((tile, cols), lambda i, place: (i, 0)),
                pl.BlockSpec((rank, tile), lambda i, place: (0, i)),
                pl.BlockSpec((rank, cols), lambda i, place: (0, 0)),
                pl.BlockSpec((4, cols), lambda i, place: (0, 0)),
            ],
            out_specs=specs,
        ),
        out_shape=shapes,
        compiler_params=pltpu.CompilerParams(vmem_limit_bytes=GRANT),
        name="own",
        cost_estimate=pl.CostEstimate(
            flops=2 * rows * cols * rank, bytes_accessed=6 * rows * cols, transcendentals=0
        ),
    )(place, train, low_t, high, factor)


def pairs_of(count, side, hop):
    pairs = []
    for i in range(count):
        to = i + 1 - 2 * ((i + side) % 2)
        owner = to + hop * (i - to)
        if 0 <= to < count and 0 <= owner < count:
            pairs.append((i, to))
    return pairs


def per_device(count, *operands):
    return merged_for_serving(count, *operands)


def merged_for_serving(
    count,
    train_query,
    low_query,
    high_query,
    train_key,
    low_key,
    high_key,
    train_value,
    low_value,
    high_value,
    norm_train,
    norm_step,
):
    rows, _ = train_query.shape
    half = rows // 2
    place = lax.axis_index("zero").astype(jnp.int32).reshape(1)
    lows = (low_query.T, low_key.T, low_value.T)
    highs = (high_query, high_key, high_value)
    trains = (train_query, train_key, train_value)

    def sent(hop, first, second):
        moved = []
        for side, x in ((0, first), (1, second)):
            pairs = pairs_of(count, side, hop)
            if pairs:
                moved.append((side, lax.ppermute(x, "zero", pairs)))
        return moved

    raw = {"q": sent(1, train_query, train_query)}
    gains = norm_train.reshape(1, -1), norm_step.reshape(1, -1)
    tops = column_tops(trains, lows, highs, gains)
    ends = {0: 1, count - 1: count - 2} if count > 2 else {0: 1}
    back = [(neighbour, end) for end, neighbour in ends.items()]
    parts = [tops]
    for s in range(1, count):
        pairs = [(i, (i + s) % count) for i in range(count) if (i + s) % count not in ends]
        parts.append(lax.ppermute(tops, "zero", pairs))
    raw["ka"] = sent(1, train_key[:half], train_key[:half])
    low = jnp.concatenate((lows[0], lows[1]), axis=1)
    whole = low.shape[1]
    devices = lax.axis_size("width")
    shared = whole % devices == 0
    if shared:
        part = whole // devices
        low = lax.dynamic_slice_in_dim(low, lax.axis_index("width") * part, part, axis=1)
    near = dict(sent(1, low, low))
    sides = sorted(near)
    joined = jnp.stack([near[side] for side in sides])
    if shared:
        joined = lax.all_gather(joined, "width", axis=2, tiled=True)
    near = {side: joined[index] for index, side in enumerate(sides)}
    joined_tops, norms = join_tops(place, parts)
    factor = jnp.maximum(joined_tops, lax.ppermute(joined_tops, "zero", back))
    raw["kb"] = sent(1, train_key[half:], train_key[half:])

    outs, serves = [None] * 3, [None] * 3
    for index, begin in ((2, 0), (1, rows), (0, rows)):
        outs[index], *serves[index] = own_scaled(
            index, place, count, trains[index], lows[index], highs[index], factor, begin
        )
    pieces = []
    for name, index, at, low_at in (("q", 0, 0, 0), ("ka", 1, 0, rows), ("kb", 1, half, rows + half)):
        arrived = []
        for side, got in raw[name]:
            arrived.append((side, scaled(index, got, near[side], highs[index], factor, low_at)))
        pieces.append((name, index, at, arrived))
    cut = rows * 3 // 4
    for name, index, at, ready in (
        ("v", 2, 0, serves[2][0][:cut]),
        ("w", 2, cut, serves[2][0][cut:]),
    ):
        pieces.append((name, index, at, sent(1, ready, ready)))

    for hop in range(1, count):
        later = []
        for name, index, at, arrived in pieces:
            if hop + 1 < count:
                brought = dict(arrived)
                later.append((name, index, at, sent(hop + 1, brought.get(1), brought.get(0))))
            outs[index] = placed(outs[index], count, hop, at, rows, arrived)
        pieces = later

    size = norm_train.shape[0]
    narrow = norms[:count, :size].astype(jnp.bfloat16)
    moved = lax.ppermute(narrow, "zero", back)
    at_end = functools.reduce(jnp.logical_or, [place == end for end in ends])
    narrow = jnp.where(at_end, moved, narrow)
    wide = lax.all_gather(narrow, "width", axis=1, tiled=True)
    serve_norm = wide.reshape(-1)
    return (*outs, factor[0], factor[1], factor[2], serve_norm)


def solution(mesh):
    count = mesh.shape["zero"]
    return jax.shard_map(
        functools.partial(per_device, count),
        mesh=mesh,
        in_specs=(
            P(("unit", "zero"), "width"),
            P(("unit", "zero"), None),
            P("unit", "width"),
            P(("unit", "zero"), "width"),
            P(("unit", "zero"), None),
            P("unit", "width"),
            P(("unit", "zero"), "width"),
            P(("unit", "zero"), None),
            P("unit", "width"),
            P(("unit", "zero", "width")),
            P(("unit", "zero", "width")),
        ),
        out_specs=(
            P("unit", "width"),
            P("unit", "width"),
            P("unit", "width"),
            P(("unit", "width")),
            P(("unit", "width")),
            P(("unit", "width")),
            P("unit"),
        ),
        check_vma=False,
    )
```
